256 devices in a mesh: rows: 32 (over y, x, core), cols: 8 (over z).
Axes of the slice: x: 4, y: 4, z: 8, core: 2. Of those that a mesh axis runs over, the one named last changes fastest.
Arguments:
- grads: bfloat16 [8192, 4096], P('rows', 'cols'), may hold values from -6 to 6
- probe: bfloat16 [8192, 4096], P('rows', 'cols'), may hold values from -6 to 6
- left_factor: float32 [8192], P('rows'), may hold values from 0.5 to 2
- q_right: float32 [4096, 4096], P('cols', 'rows'), may hold values from -1 to 2
- q_inv_t: float32 [4096, 4096], P('cols', 'rows'), may hold values from -1 to 2
Outputs:
- left_new: float32 [8192], P('rows')
- q_new: float32 [4096, 4096], P('cols', 'rows')
The draws below stay inside these ranges and needn't reach their ends.
All inputs are finite; a program needn't handle non-finite values. Where the reference program divides by a largest or mean magnitude, that divisor is 1e-20 or more.
Results may differ from the reference program's by a relative error of at most 0.0058.
Values may be sent and summed in bfloat16 or wider, within the bound.
No kernel may reach another device: no remote copies, remote signals or barrier semaphores. Data moves between devices by JAX's collectives and lax.ppermute only.
A program may use at most 64 MiB of HBM per device.

```python
import math
import jax
import jax.numpy as jnp
from jax import lax

D = 4096
VOCAB = 8192


def factor_draw(key, salt):
    noise = jax.random.normal(jax.random.fold_in(key, salt), (D, D), jnp.float32)
    noise = jnp.clip(noise, -6.0, 6.0)
    return jnp.eye(D, dtype=jnp.float32) + 0.5 * noise / jnp.sqrt(jnp.float32(D))


def draw_q_right(key, part):
    return factor_draw(key, 11)


def draw_q_inv_t(key, part):
    return factor_draw(key, 23)


def shard_levels(own_key, shape, cuts, least, top_value):
    loudness, own = 1.0, jax.random.fold_in(own_key, 6)
    for position, parts in cuts:
        steps = jnp.exp(jax.random.uniform(jax.random.fold_in(own, position), (parts,), jnp.float32, least / len(cuts), top_value / len(cuts)))
        loudness = loudness * jnp.repeat(steps, shape[position] // parts).reshape([-1 if axis == position else 1 for axis in range(len(shape))])
    return loudness


def centred(key, extent, scale, bound, shards=(), held_as=jnp.bfloat16):
    array = jax.random.normal(key, extent, jnp.float32) * scale
    if len(shards) > 0:
        array = shard_levels(key, extent, shards, -0.22, 0.18) * array
    return jnp.clip(array, min=-bound, max=bound).astype(held_as)


def setup_inputs(seed: int = 0) -> dict:
    key_list = jax.random.split(jax.random.key(seed), 6)
    return {
        "grads": centred(key_list[0], (VOCAB, D), 1.0, 6.0, ((0, 32), (1, 8))),
        "probe": centred(key_list[1], (VOCAB, D), 1.0, 6.0, ((0, 32), (1, 8))),
        "left_factor": jnp.clip(jnp.exp(math.log(2.0) - 1.3862944 * jax.random.uniform(key_list[2], (VOCAB,), jnp.float32) ** shard_levels(key_list[2], (VOCAB,), ((0, 32),), -0.2, 0.2)), 0.5, 2.0),
        "q_right": draw_q_right(jax.random.fold_in(key_list[5], 71), 0),
        "q_inv_t": draw_q_inv_t(jax.random.fold_in(key_list[5], 71), 0),
    }


learn_rate = 0.2
epsilon = 1e-6


def reference(grads, probe, left_factor, q_right, q_inv_t):
    q_low = q_right.astype(jnp.bfloat16)
    inv_low = q_inv_t.astype(jnp.bfloat16)
    white = (left_factor[:, None] * jnp.dot(grads, q_low.T, preferred_element_type=jnp.float32)).astype(jnp.bfloat16)
    conj = ((1.0 / left_factor)[:, None] * jnp.dot(probe, inv_low.T, preferred_element_type=jnp.float32)).astype(jnp.bfloat16)
    white_f = white.astype(jnp.float32)
    conj_f = conj.astype(jnp.float32)
    left_grad = jnp.sum(white_f * white_f - conj_f * conj_f, axis=1)
    gram = jnp.dot(white.T, white, preferred_element_type=jnp.float32) - jnp.dot(conj.T, conj, preferred_element_type=jnp.float32)
    scale_r = learn_rate / (jnp.max(jnp.abs(gram)) + epsilon)
    scale_l = learn_rate / (jnp.max(jnp.abs(left_grad)) + epsilon)
    left_new = left_factor - scale_l * left_grad * left_factor
    q_new = q_right - scale_r * jnp.dot(gram, q_right, precision=lax.Precision.HIGHEST)
    return left_new, q_new
```

```python
import jax
import jax.numpy as jnp
from jax import lax
from jax.sharding import Mesh
from jax.sharding import PartitionSpec as P

ROWS = ("rows_0", "rows_1", "rows_2")
PLANE = ("rows_0", "rows_1")
CORE = "rows_2"
COLS = "cols"


learn_rate = 0.2
epsilon = 1e-06
f32 = jnp.float32
bf16 = jnp.bfloat16


def shift(value, axis, by):
    size = lax.axis_size(axis)
    return lax.ppermute(value, axis, [(i, (i + by) % size) for i in range(size)])


def ring_gather(value, axis):
    size, me = lax.axis_size(axis), lax.axis_index(axis)
    rows, width = value.shape
    full = jnp.zeros((rows, size * width), value.dtype)

    def put(full, block, owner, row):
        return lax.dynamic_update_slice(full, block, (row, ((owner + size) % size) * width))

    full = put(full, value, me, 0)
    up = down = value
    for step in range(1, size // 2):
        up, down = shift(up, axis, 1), shift(down, axis, -1)
        full = put(put(full, up, me - step, 0), down, me + step, 0)
    half = rows // 2
    last_up, last_down = shift(up[:half], axis, 1), shift(down[half:], axis, -1)
    opposite = me + size // 2
    return put(put(full, last_up, opposite, 0), last_down, opposite, half)


def from_everyone(value, axes):
    size = lax.axis_size(axes)
    copies = jnp.broadcast_to(value[None], (size, *value.shape))
    return lax.all_to_all(copies, axes, 0, 0, tiled=True)


def dot(left, right, left_dim, right_dim):
    return lax.dot_general(
        left, right, (((left_dim,), (right_dim,)), ((), ())), preferred_element_type=f32
    )


def body(grads, probe, left_factor, q_right, q_inv_t):
    n_cols, me = lax.axis_size(COLS), lax.axis_index(COLS)
    core = lax.axis_index(CORE)
    n_rows = lax.axis_size(ROWS)
    n_plane = lax.axis_size(PLANE)
    width = grads.shape[1]

    q_low = q_right.astype(bf16)
    inv_low = q_inv_t.astype(bf16)
    both = lax.all_gather(
        jnp.concatenate([q_low.T, inv_low.T], axis=1), ROWS, axis=0, tiled=True
    )
    grad_full, probe_full = ring_gather(grads, COLS), ring_gather(probe, COLS)
    q_all = lax.all_gather(q_low, COLS, axis=0, tiled=True)

    white = (left_factor[:, None] * dot(grad_full, both[:, :width], 1, 0)).astype(bf16)
    conj = ((1.0 / left_factor)[:, None] * dot(probe_full, both[:, width:], 1, 0)).astype(bf16)
    white_f, conj_f = white.astype(f32), conj.astype(f32)
    left_part = jnp.sum(white_f * white_f - conj_f * conj_f, axis=1)

    own = jnp.concatenate([white, conj], axis=0)
    near = {0: own, -1: shift(own, COLS, 1), 1: shift(own, COLS, -1)}
    near[-2], near[2] = shift(near[-1], COLS, 1), shift(near[1], COLS, -1)
    n_own = white.shape[0]

    def pair(a, b):
        signed = jnp.concatenate([near[b][:n_own], -near[b][n_own:]], axis=0)
        return dot(near[a], signed, 0, 0)

    pairs = [pair(0, 0), pair(0, 1), pair(-1, 1), pair(-1, 2), pair(-2, 2)]
    part = jnp.concatenate(pairs, axis=1)
    piece = width // n_rows
    part = part.reshape(n_plane, 2, piece, part.shape[1])
    keep = lax.dynamic_index_in_dim(part, core, 1, keepdims=False)
    give = lax.dynamic_index_in_dim(part, 1 - core, 1, keepdims=False).astype(bf16)
    part = (keep + shift(give, CORE, 1).astype(f32)).astype(bf16)
    parts = lax.all_to_all(part, PLANE, 0, 0, tiled=True)
    total = jnp.sum(parts.astype(f32), axis=0)

    top_r = jnp.max(jnp.abs(total))
    low = total.astype(bf16)
    d0, d1, d2, d3, d4 = (low[:, i * width : (i + 1) * width] for i in range(5))
    above = shift(jnp.concatenate([d2, d3], axis=1), COLS, -1)
    below = shift(jnp.concatenate([d1, d2], axis=1), COLS, 1)
    above_2, below_2 = shift(d4, COLS, -2), shift(d3, COLS, 2)
    slices = jnp.concatenate([d0, d1, above, above_2, below, below_2], axis=1)
    gram = lax.all_gather(slices, ROWS, axis=0, tiled=True)

    note = jnp.concatenate([left_part, jnp.full((width,), top_r)]).reshape(-1, 128)
    notes = from_everyone(note, COLS).reshape(n_cols, -1)
    left_grad = jnp.sum(notes[:, :n_own], axis=0)
    tops = jnp.stack([jnp.max(notes[:, n_own:]), jnp.max(jnp.abs(left_grad))])
    tops = from_everyone(jnp.broadcast_to(tops[:, None, None], (2, 8, 128)), ROWS)
    top_r, top_l = jnp.max(tops[:, 0]), jnp.max(tops[:, 1])
    scale_r = learn_rate / (top_r + epsilon)
    scale_l = learn_rate / (top_l + epsilon)
    left_new = left_factor - scale_l * left_grad * left_factor

    q_near = lax.dynamic_slice_in_dim(
        jnp.concatenate([q_all, q_all], axis=0), me * width, n_cols * width, axis=0
    )
    ahead = 5 * width
    product = dot(gram[:, :ahead], q_near[:ahead], 1, 0)
    for i in range(3):
        at = (n_cols - 1 - i) * width
        block = gram[:, ahead + i * width : ahead + (i + 1) * width]
        product = product + dot(block, q_near[at : at + width], 0, 0)
    q_new = q_right - scale_r * product
    return (left_new, q_new)


def solution(mesh):
    finer = Mesh(
        mesh.devices.reshape(4, 4, 2, mesh.shape["cols"]), ("rows_0", "rows_1", "rows_2", "cols")
    )
    in_specs = (P(ROWS, "cols"), P(ROWS, "cols"), P(ROWS), P("cols", ROWS), P("cols", ROWS))
    out_specs = (P(ROWS), P("cols", ROWS))
    return jax.shard_map(body, mesh=finer, in_specs=in_specs, out_specs=out_specs, check_vma=False)
```

```python
import jax
import jax.numpy as jnp
from jax import lax
from jax.sharding import Mesh
from jax.sharding import PartitionSpec as P

ROWS = ("rows_0", "rows_1", "rows_2")
PLANE = ("rows_0", "rows_1")
CORE = "rows_2"
COLS = "cols"


learn_rate = 0.2
epsilon = 1e-06
f32 = jnp.float32
bf16 = jnp.bfloat16


def shift(value, axis, by):
    size = lax.axis_size(axis)
    return lax.ppermute(value, axis, [(i, (i + by) % size) for i in range(size)])


def from_everyone(value, axes):
    size = lax.axis_size(axes)
    copies = jnp.broadcast_to(value[None], (size, *value.shape))
    return lax.all_to_all(copies, axes, 0, 0, tiled=True)


def dot(left, right, left_dim, right_dim):
    return lax.dot_general(
        left, right, (((left_dim,), (right_dim,)), ((), ())), preferred_element_type=f32
    )


def ring_gather(value):
    size, me = lax.axis_size(COLS), lax.axis_index(COLS)
    rows, width = value.shape[0], value.shape[1] // 2
    fulls = [jnp.zeros((rows, size * width), value.dtype) for _ in range(2)]

    def put(block, owner, row):
        at = ((owner + size) % size) * width
        for i in range(2):
            part = block[:, i * width : (i + 1) * width]
            fulls[i] = lax.dynamic_update_slice(fulls[i], part, (row, at))

    put(value, me, 0)
    up = down = value
    for step in range(1, size // 2):
        up, down = shift(up, COLS, 1), shift(down, COLS, -1)
        put(up, me - step, 0)
        put(down, me + step, 0)
    half = rows // 2
    put(shift(up[:half], COLS, 1), me + size // 2, 0)
    put(shift(down[half:], COLS, -1), me + size // 2, half)
    return fulls


def split(value):
    high = lax.reduce_precision(value, 8, 7)
    middle = lax.reduce_precision(value - high, 8, 7)
    return [t.astype(bf16) for t in (high, middle, value - high - middle)]


def joined(terms):
    terms = terms.astype(f32)
    return (terms[..., 0] + terms[..., 1]) + terms[..., 2]


def note_of(values, rows):
    terms = jnp.stack([t for v in values for t in split(v)])
    return jnp.broadcast_to(jnp.pad(terms, (0, 128 - terms.shape[0]))[None], (rows, 128))


def after(value, *others):
    return lax.optimization_barrier((value, *others))[0]


def body(grads, probe, left_factor, q_right, q_inv_t):
    n_cols, me = lax.axis_size(COLS), lax.axis_index(COLS)
    core = lax.axis_index(CORE)
    n_plane = lax.axis_size(PLANE)
    height, width = grads.shape
    strip = q_right.shape[1]

    q_low = q_right.astype(bf16)
    inv_low = q_inv_t.astype(bf16)

    def own_first(value):
        strips = value.reshape(height, width // (2 * strip), 2, strip)
        mine = lax.dynamic_index_in_dim(strips, core, 2, keepdims=False)
        others = lax.dynamic_index_in_dim(strips, 1 - core, 2, keepdims=False)
        return jnp.concatenate([v.reshape(height, width // 2) for v in (mine, others)], axis=1)

    def over_plane(value, first, second):
        return from_everyone(from_everyone(value, first), second)

    q_mine = over_plane(q_low.T, "rows_1", "rows_0").reshape(n_plane * strip, width)
    inv_mine = over_plane(inv_low.T, "rows_0", "rows_1")
    inv_mine = jnp.swapaxes(inv_mine, 0, 1).reshape(n_plane * strip, width)
    grad_fulls, probe_fulls = ring_gather(own_first(grads)), ring_gather(own_first(probe))
    q_other, inv_other = shift(q_mine, CORE, 1), shift(inv_mine, CORE, 1)

    def whitened(scale, fulls, mine, other):
        product = dot(fulls[0], mine, 1, 0) + dot(fulls[1], other, 1, 0)
        return (scale[:, None] * product).astype(bf16)

    white = whitened(left_factor, grad_fulls, q_mine, q_other)
    conj = whitened(1.0 / left_factor, probe_fulls, inv_mine, inv_other)

    own = jnp.concatenate([white, conj], axis=0)
    near = {0: own, -1: shift(own, COLS, 1), 1: shift(own, COLS, -1)}
    near[-2], near[2] = shift(near[-1], COLS, 1), shift(near[1], COLS, -1)

    def pair(a, b):
        signed = jnp.concatenate([near[b][:height], -near[b][height:]], axis=0)
        return dot(near[a], signed, 0, 0)

    half = width // 2
    piece = half // n_plane

    def over_rows(pairs):
        part = jnp.concatenate([pair(a, b) for a, b in pairs], axis=1)
        keep = lax.dynamic_slice_in_dim(part, core * half, half, axis=0)
        give = lax.dynamic_slice_in_dim(part, (1 - core) * half, half, axis=0).astype(bf16)
        part = (keep + shift(give, CORE, 1).astype(f32)).astype(bf16)
        part = part.reshape(n_plane, piece, part.shape[1])
        parts = lax.all_to_all(part, PLANE, 0, 0, tiled=True)
        return jnp.sum(parts.astype(f32), axis=0)

    early = over_rows([(0, 0), (0, 1), (-1, 1)])
    late = over_rows([(-1, 2), (-2, 2)])

    white_l, conj_l, _ = lax.optimization_barrier((white, conj, near[1]))
    white_f, conj_f = white_l.astype(f32), conj_l.astype(f32)
    left_part = jnp.sum(white_f * white_f - conj_f * conj_f, axis=1)
    left_grad = jnp.sum(from_everyone(left_part.reshape(-1, 128), COLS).reshape(n_cols, -1), axis=0)
    top_l = jnp.max(jnp.abs(left_grad))

    q_all = from_everyone(after(q_low, near[2]), COLS).reshape(n_cols * width, strip)
    q_both = jnp.concatenate([q_all, shift(q_all, CORE, 1)], axis=1)
    q_near = lax.dynamic_slice_in_dim(
        jnp.concatenate([q_both, q_both], axis=0), me * width, n_cols * width, axis=0
    )

    top_r = jnp.maximum(jnp.max(jnp.abs(early)), jnp.max(jnp.abs(late)))
    d0, d1, d2 = (early[:, i * width : (i + 1) * width].astype(bf16) for i in range(3))
    d3, d4 = (late[:, i * width : (i + 1) * width].astype(bf16) for i in range(2))
    note = note_of([top_r], piece)
    above = shift(jnp.concatenate([d2, d3, note], axis=1), COLS, -1)
    below = shift(jnp.concatenate([d1, d2, note], axis=1), COLS, 1)
    above_2 = shift(jnp.concatenate([d4, note], axis=1), COLS, -2)
    below_2 = shift(jnp.concatenate([d3, note], axis=1), COLS, 2)
    for sent in (above, below, above_2, below_2):
        top_r = jnp.maximum(top_r, joined(sent[0, -128:-125]))
    blocks = [d0, d1, above[:, :-128], above_2[:, :-128], below[:, :-128], below_2[:, :-128]]
    slices = jnp.concatenate([*blocks, note_of([top_r, top_l], piece)], axis=1)
    gram = from_everyone(slices, PLANE)

    top_r = jnp.max(joined(gram[:, 0, n_cols * width : n_cols * width + 3]))
    top_l = jnp.max(joined(gram[:, 0, n_cols * width + 3 : n_cols * width + 6]))
    tops = jnp.broadcast_to(jnp.stack([top_r, top_l])[:, None], (2, 128))
    tops_core = shift(tops, CORE, 1)
    tops = jnp.maximum(tops, tops_core)
    top_l = tops[1, 0]
    top_r = jnp.maximum(tops, shift(tops, COLS, n_cols // 2))[0, 0]
    scale_r = learn_rate / (top_r + epsilon)
    scale_l = learn_rate / (top_l + epsilon)
    left_new = left_factor - scale_l * left_grad * left_factor

    gram = gram.reshape(n_plane * piece, -1)
    ahead = 5 * width
    straight = dot(gram[:, :ahead], q_near[:ahead], 1, 0)
    turned = []
    for i in range(3):
        at = (n_cols - 1 - i) * width + core * half
        block = gram[:, ahead + i * width : ahead + (i + 1) * width]
        turned.append(dot(block, lax.dynamic_slice_in_dim(q_near, at, half, axis=0), 0, 0))
    product = turned[0] + turned[1] + turned[2]
    rows = lax.dynamic_slice_in_dim(product, core * half, half, axis=0) + straight
    product = lax.dynamic_update_slice_in_dim(product, rows, core * half, axis=0)
    product = product[:, :strip] + shift(product[:, strip:], CORE, 1)
    q_new = q_right - scale_r * product
    return (left_new, q_new)


def solution(mesh):
    finer = Mesh(
        mesh.devices.reshape(4, 4, 2, mesh.shape["cols"]), ("rows_0", "rows_1", "rows_2", "cols")
    )
    in_specs = (P(ROWS, "cols"), P(ROWS, "cols"), P(ROWS), P("cols", ROWS), P("cols", ROWS))
    out_specs = (P(ROWS), P("cols", ROWS))
    return jax.shard_map(body, mesh=finer, in_specs=in_specs, out_specs=out_specs, check_vma=False)
```

```python
import jax
import jax.numpy as jnp
from jax import lax
from jax.experimental.layout import Layout, with_layout_constraint
from jax.sharding import Mesh
from jax.sharding import PartitionSpec as P

ROWS = ("rows_0", "rows_1", "rows_2")
PLANE = ("rows_0", "rows_1")
CORE = "rows_2"
COLS = "cols"


learn_rate = 0.2
epsilon = 1e-06
f32 = jnp.float32
bf16 = jnp.bfloat16


def shift(value, axis, by):
    size = lax.axis_size(axis)
    return lax.ppermute(value, axis, [(i, (i + by) % size) for i in range(size)])


def ring_gather(value, axis, put, result, half_dim):
    size, me = lax.axis_size(axis), lax.axis_index(axis)
    result = put(result, value, me, 0)
    up = down = value
    for step in range(1, size // 2):
        up, down = shift(up, axis, 1), shift(down, axis, -1)
        result = put(result, up, (me - step + size) % size, 0)
        result = put(result, down, (me + step) % size, 0)
    half = value.shape[half_dim] // 2
    first = lax.slice_in_dim(up, 0, half, axis=half_dim)
    second = lax.slice_in_dim(down, half, 2 * half, axis=half_dim)
    opposite = (me + size // 2) % size
    result = put(result, shift(first, axis, 1), opposite, 0)
    return put(result, shift(second, axis, -1), opposite, half)


def gather_plane(value, first, second):
    n_0, n_1 = (lax.axis_size(axis) for axis in PLANE)

    def put_line(line, block, owner, row):
        return lax.dynamic_update_slice(line, block[None], (owner, row, 0))

    def put_plane(plane, block, owner, begin):
        if second == PLANE[0]:
            return lax.dynamic_update_slice(plane, block[None], (owner, begin, 0, 0))
        return lax.dynamic_update_slice(plane, block[:, None], (begin, owner, 0, 0))

    line = jnp.zeros((lax.axis_size(first), *value.shape), value.dtype)
    size, me = lax.axis_size(first), lax.axis_index(first)
    line = put_line(line, value, me, 0)
    for by in (1, -1, 2):
        line = put_line(line, shift(value, first, by), (me - by + size) % size, 0)
    plane = jnp.zeros((n_0, n_1, *value.shape), value.dtype)
    return ring_gather(line, second, put_plane, plane, 0)


def from_everyone(value, axes):
    size = lax.axis_size(axes)
    copies = jnp.broadcast_to(value[None], (size, *value.shape))
    return lax.all_to_all(copies, axes, 0, 0, tiled=True)


def from_both_cores(plane):
    n_0, n_1, strip, width = plane.shape
    core = lax.axis_index(CORE)
    whole = jnp.zeros((n_0, n_1, 2, strip, width), plane.dtype)
    whole = lax.dynamic_update_slice(whole, plane[:, :, None], (0, 0, core, 0, 0))
    other = shift(plane, CORE, 1)
    whole = lax.dynamic_update_slice(whole, other[:, :, None], (0, 0, 1 - core, 0, 0))
    return whole.reshape(n_0 * n_1 * 2 * strip, width)


def dot(left, right, left_dim, right_dim):
    return lax.dot_general(
        left, right, (((left_dim,), (right_dim,)), ((), ())), preferred_element_type=f32
    )


def after(values, *others):
    return lax.optimization_barrier((values, *others))[0]


def body(grads, probe, left_factor, q_right, q_inv_t):
    n_cols, me = lax.axis_size(COLS), lax.axis_index(COLS)
    core = lax.axis_index(CORE)
    n_plane = lax.axis_size(PLANE)
    height, width = grads.shape
    half = width // 2
    piece = half // n_plane

    q_low = q_right.astype(bf16)
    inv_low = q_inv_t.astype(bf16)
    both = lax.all_gather(jnp.concatenate([grads, probe], axis=0), COLS, axis=1, tiled=True)
    q_rows = from_both_cores(gather_plane(q_low.T, "rows_1", "rows_0"))
    inv_rows = from_both_cores(gather_plane(inv_low.T, "rows_0", "rows_1"))

    white = (left_factor[:, None] * dot(both[:height], q_rows, 1, 0)).astype(bf16)
    conj = ((1.0 / left_factor)[:, None] * dot(both[height:], inv_rows, 1, 0)).astype(bf16)

    own = jnp.concatenate([white, conj], axis=0)
    before, behind = shift(own, COLS, 1), shift(own, COLS, -1)
    before_2, behind_2 = shift(before, COLS, 1), shift(behind, COLS, -1)

    def pair(left, right):
        signed = jnp.concatenate([right[:height], -right[height:]], axis=0)
        return with_layout_constraint(dot(left, signed, 0, 0), Layout(major_to_minor=(0, 1)))

    def over_cores(pairs):
        part = jnp.concatenate([pair(a, b) for a, b in pairs], axis=1)
        keep = lax.dynamic_slice_in_dim(part, core * half, half, axis=0)
        give = lax.dynamic_slice_in_dim(part, (1 - core) * half, half, axis=0).astype(bf16)
        part = (keep + shift(give, CORE, 1).astype(f32)).astype(bf16)
        return part.reshape(n_plane, piece, part.shape[1])

    def over_plane(part):
        return jnp.sum(lax.all_to_all(part, PLANE, 0, 0, tiled=True).astype(f32), axis=0)

    early_part = over_cores([(own, own), (own, behind), (before, behind)])
    before_2, behind_2, white, conj, early_part = lax.optimization_barrier(
        (before_2, behind_2, white, conj, early_part)
    )
    early = over_plane(early_part)
    late = over_plane(over_cores([(before, behind_2), (before_2, behind_2)]))

    white_f, conj_f = white.astype(f32), conj.astype(f32)
    left_part = jnp.sum(white_f * white_f - conj_f * conj_f, axis=1)
    q_all = lax.all_gather(after(q_low, behind_2), COLS, axis=0, tiled=True)

    d0, d1, d2 = (early[:, i * width : (i + 1) * width].astype(bf16) for i in range(3))
    d3, d4 = (late[:, i * width : (i + 1) * width].astype(bf16) for i in range(2))
    above = shift(jnp.concatenate([d2, d3], axis=1), COLS, -1)
    below = shift(jnp.concatenate([d1, d2], axis=1), COLS, 1)
    above_2, below_2 = shift(d4, COLS, -2), shift(d3, COLS, 2)
    slices = jnp.concatenate([d0, d1, above, above_2, below, below_2], axis=1)
    gram = lax.all_gather(slices, ROWS, axis=0, tiled=True)

    top_r = jnp.maximum(jnp.max(jnp.abs(early)), jnp.max(jnp.abs(late)))
    note = jnp.concatenate([left_part, jnp.full((width,), top_r)]).reshape(-1, 128)
    notes = from_everyone(note, COLS).reshape(n_cols, -1)
    left_grad = jnp.sum(notes[:, :height], axis=0)
    tops = jnp.stack([jnp.max(notes[:, height:]), jnp.max(jnp.abs(left_grad))])
    tops = from_everyone(jnp.broadcast_to(tops[:, None, None], (2, 8, 128)), ROWS)
    top_r, top_l = jnp.max(tops[:, 0]), jnp.max(tops[:, 1])
    scale_r = learn_rate / (top_r + epsilon)
    scale_l = learn_rate / (top_l + epsilon)
    left_new = left_factor - scale_l * left_grad * left_factor

    ahead = 5 * width
    q_near = lax.dynamic_slice_in_dim(
        jnp.concatenate([q_all, q_all], axis=0), me * width, n_cols * width, axis=0
    )
    product = dot(gram[:, :ahead], q_near[:ahead], 1, 0)
    product = jnp.swapaxes(product.reshape(n_plane, 2, piece, -1), 0, 1).reshape(width, -1)
    for i in range(3):
        at = (n_cols - 1 - i) * width
        rows = q_near[at : at + width].reshape(2, n_plane, piece, -1)
        rows = jnp.swapaxes(rows, 0, 1).reshape(width, -1)
        block = gram[:, ahead + i * width : ahead + (i + 1) * width]
        product = product + dot(block, rows, 0, 0)
    q_new = q_right - scale_r * product
    return (left_new, q_new)


def solution(mesh):
    finer = Mesh(
        mesh.devices.reshape(4, 4, 2, mesh.shape["cols"]), ("rows_0", "rows_1", "rows_2", "cols")
    )
    in_specs = (P(ROWS, "cols"), P(ROWS, "cols"), P(ROWS), P("cols", ROWS), P("cols", ROWS))
    out_specs = (P(ROWS), P("cols", ROWS))
    return jax.shard_map(body, mesh=finer, in_specs=in_specs, out_specs=out_specs, check_vma=False)
```

```python
import jax
import jax.numpy as jnp
from jax import lax
from jax.experimental.layout import Layout, with_layout_constraint
from jax.sharding import Mesh
from jax.sharding import PartitionSpec as P

ROWS = ("rows_0", "rows_1", "rows_2")
PLANE = ("rows_0", "rows_1")
CORE = "rows_2"
COLS = "cols"


learn_rate = 0.2
epsilon = 1e-06
NOTE_ROWS = 16
f32 = jnp.float32
bf16 = jnp.bfloat16


def shift(value, axis, by):
    size = lax.axis_size(axis)
    return lax.ppermute(value, axis, [(i, (i + by) % size) for i in range(size)])


def ring_gather(value, axis, put, result, half_dim):
    size, me = lax.axis_size(axis), lax.axis_index(axis)
    result = put(result, value, me, 0)
    up = down = value
    for step in range(1, size // 2):
        up, down = shift(up, axis, 1), shift(down, axis, -1)
        result = put(result, up, (me - step + size) % size, 0)
        result = put(result, down, (me + step) % size, 0)
    half = value.shape[half_dim] // 2
    first = lax.slice_in_dim(up, 0, half, axis=half_dim)
    second = lax.slice_in_dim(down, half, 2 * half, axis=half_dim)
    opposite = (me + size // 2) % size
    result = put(result, shift(first, axis, 1), opposite, 0)
    return put(result, shift(second, axis, -1), opposite, half)


def gather_plane(value, first, second):
    n_0, n_1 = (lax.axis_size(axis) for axis in PLANE)

    def put_line(line, block, owner, row):
        return lax.dynamic_update_slice(line, block[None], (owner, row, 0))

    def put_plane(plane, block, owner, begin):
        if second == PLANE[0]:
            return lax.dynamic_update_slice(plane, block[None], (owner, begin, 0, 0))
        return lax.dynamic_update_slice(plane, block[:, None], (begin, owner, 0, 0))

    line = jnp.zeros((lax.axis_size(first), *value.shape), value.dtype)
    size, me = lax.axis_size(first), lax.axis_index(first)
    line = put_line(line, value, me, 0)
    for by in (1, -1, 2):
        line = put_line(line, shift(value, first, by), (me - by + size) % size, 0)
    plane = jnp.zeros((n_0, n_1, *value.shape), value.dtype)
    return ring_gather(line, second, put_plane, plane, 0)


def from_everyone(value, axes):
    size = lax.axis_size(axes)
    copies = jnp.broadcast_to(value[None], (size, *value.shape))
    return lax.all_to_all(copies, axes, 0, 0, tiled=True)


def dot(left, right, left_dim, right_dim):
    return lax.dot_general(
        left, right, (((left_dim,), (right_dim,)), ((), ())), preferred_element_type=f32
    )


def turned(values, by):
    size = values.shape[0]
    twice = jnp.concatenate([values, values], axis=0)
    return lax.dynamic_slice_in_dim(twice, (by + size) % size, size, axis=0)


def split(value):
    high = lax.reduce_precision(value, 8, 7)
    middle = lax.reduce_precision(value - high, 8, 7)
    return [t.astype(bf16) for t in (high, middle, value - high - middle)]


def after(values, *others):
    return lax.optimization_barrier((values, *others))[0]


def body(grads, probe, left_factor, q_right, q_inv_t):
    n_cols, me = lax.axis_size(COLS), lax.axis_index(COLS)
    core = lax.axis_index(CORE)
    n_plane = lax.axis_size(PLANE)
    height, width = grads.shape
    half = width // 2
    piece = half // n_plane

    q_low = q_right.astype(bf16)
    inv_low = q_inv_t.astype(bf16)
    both = lax.all_gather(jnp.concatenate([grads, probe], axis=0), COLS, axis=1, tiled=True)

    def half_of(value, which):
        return lax.dynamic_slice_in_dim(value, which * half, half, axis=1)

    def in_core_order(mine, others, axis):
        first = jnp.concatenate([mine, others], axis=axis)
        second = jnp.concatenate([others, mine], axis=axis)
        return jnp.where(core == 0, first, second)

    q_t, inv_t = q_low.T, inv_low.T
    got = shift(jnp.concatenate([half_of(q_t, 1 - core), half_of(inv_t, 1 - core)], axis=1), CORE, 1)
    q_pair = in_core_order(half_of(q_t, core), got[:, :half], 0)
    inv_pair = in_core_order(half_of(inv_t, core), got[:, half:], 0)
    q_half = gather_plane(q_pair, "rows_1", "rows_0").reshape(-1, half)
    inv_half = gather_plane(inv_pair, "rows_0", "rows_1").reshape(-1, half)
    q_other, inv_other = shift(q_half, CORE, 1), shift(inv_half, CORE, 1)

    def whitened(scale, values, mine, others):
        parts = [(scale[:, None] * dot(values, q, 1, 0)).astype(bf16) for q in (mine, others)]
        return in_core_order(*parts, 1)

    white = whitened(left_factor, both[:height], q_half, q_other)
    conj = whitened(1.0 / left_factor, both[height:], inv_half, inv_other)

    own = jnp.concatenate([white, conj], axis=0)
    before, behind = shift(own, COLS, 1), shift(own, COLS, -1)
    before_2 = shift(before, COLS, 1)
    behind_2 = shift(behind, COLS, -1)

    def pair(left, right):
        signed = jnp.concatenate([right[:height], -right[height:]], axis=0)
        return with_layout_constraint(dot(left, signed, 0, 0), Layout(major_to_minor=(0, 1)))

    def over_cores(pairs):
        products = []
        for a, b in pairs:
            products.append(pair(a, b))
        part = jnp.concatenate(products, axis=1)
        keep = lax.dynamic_slice_in_dim(part, core * half, half, axis=0)
        give = lax.dynamic_slice_in_dim(part, (1 - core) * half, half, axis=0).astype(bf16)
        got = shift(give, CORE, 1)
        part = (keep + got.astype(f32)).astype(bf16)
        return part.reshape(n_plane, piece, part.shape[1])

    def over_plane(part):
        parts = lax.all_to_all(part, PLANE, 0, 0, tiled=True)
        return jnp.sum(parts.astype(f32), axis=0)

    early_part = over_cores([(own, own), (own, behind), (before, behind)])
    early = over_plane(early_part)
    before_2, behind_2, white, conj, _ = lax.optimization_barrier(
        (before_2, behind_2, white, conj, early_part)
    )
    late_part = over_cores([(before, behind_2), (before_2, behind_2)])
    late = over_plane(late_part)

    white_f, conj_f = white.astype(f32), conj.astype(f32)
    left_part = jnp.sum(white_f * white_f - conj_f * conj_f, axis=1)
    q_all = lax.all_gather(after(q_low, late_part), COLS, axis=0, tiled=True)

    top_r = jnp.maximum(jnp.max(jnp.abs(early)), jnp.max(jnp.abs(late)))
    d0, d1, d2 = (early[:, i * width : (i + 1) * width].astype(bf16) for i in range(3))
    d3, d4 = (late[:, i * width : (i + 1) * width].astype(bf16) for i in range(2))
    way = ((jnp.arange(n_cols) - me + n_cols) % n_cols)[:, None, None]

    def by_way(choices):
        out = jnp.zeros((n_cols, *d0.shape), bf16)
        for i, value in choices.items():
            out = jnp.where(way == i % n_cols, value[None], out)
        return out

    sent = [by_way({1: d1, -1: d2, 2: d3, -2: d4}), by_way({1: d2, -1: d3})]
    terms = split(jnp.concatenate([left_part, jnp.full((128,), top_r)]))
    note = jnp.concatenate([t.reshape(-1, 128) for t in terms], axis=0)
    note = jnp.pad(note, ((0, NOTE_ROWS - note.shape[0]), (0, 0)))
    note = note.reshape(piece, -1)
    note = jnp.broadcast_to(note[None], (n_cols, *note.shape))
    blocks = lax.all_to_all(
        jnp.concatenate([*sent, note], axis=2), COLS, 0, 0, tiled=True
    )

    def got(by, size):
        block = lax.dynamic_index_in_dim(blocks, (me + by + n_cols) % n_cols, 0, keepdims=False)
        return block[:, :size]

    above, above_2 = got(1, 2 * width), got(2, width)
    below, below_2 = got(-1, 2 * width), got(-2, width)
    slices = jnp.concatenate([d0, d1, above, above_2, below, below_2], axis=1)
    gram = lax.all_gather(slices, (CORE, *PLANE), axis=0, tiled=True)

    lines = height // 128 + 1
    notes = blocks[:, :, 2 * width :].reshape(n_cols, NOTE_ROWS, 128).astype(f32)
    notes = (notes[:, :lines] + notes[:, lines : 2 * lines]) + notes[:, 2 * lines : 3 * lines]
    left_grad = jnp.sum(notes[:, :-1].reshape(n_cols, -1), axis=0)
    tops = jnp.stack([jnp.max(notes[:, -1]), jnp.max(jnp.abs(left_grad))])
    tops = from_everyone(jnp.broadcast_to(tops[:, None, None], (2, 8, 128)), ROWS)
    top_r, top_l = jnp.max(tops[:, 0]), jnp.max(tops[:, 1])
    scale_r = learn_rate / (top_r + epsilon)
    scale_l = learn_rate / (top_l + epsilon)
    left_new = left_factor - scale_l * left_grad * left_factor

    q_near = turned(q_all.reshape(n_cols, width, -1), me).reshape(n_cols * width, -1)
    ahead = 5 * width
    product = dot(gram[:, :ahead], q_near[:ahead], 1, 0)
    for i in range(3):
        at = (n_cols - 1 - i) * width
        block = gram[:, ahead + i * width : ahead + (i + 1) * width]
        product = product + dot(block, q_near[at : at + width], 0, 0)
    q_new = q_right - scale_r * product
    return (left_new, q_new)


def solution(mesh):
    finer = Mesh(
        mesh.devices.reshape(4, 4, 2, mesh.shape["cols"]), ("rows_0", "rows_1", "rows_2", "cols")
    )
    in_specs = (P(ROWS, "cols"), P(ROWS, "cols"), P(ROWS), P("cols", ROWS), P("cols", ROWS))
    out_specs = (P(ROWS), P("cols", ROWS))

    return jax.shard_map(body, mesh=finer, in_specs=in_specs, out_specs=out_specs, check_vma=False)
```

```python
import jax
import jax.numpy as jnp
from jax import lax
from jax.experimental import pallas as pl
from jax.experimental.layout import Layout, with_layout_constraint
from jax.experimental.pallas import tpu as pltpu
from jax.sharding import Mesh
from jax.sharding import PartitionSpec as P

ROWS = ("rows_0", "rows_1", "rows_2")
PLANE = ("rows_0", "rows_1")
CORE = "rows_2"
COLS = "cols"


learn_rate = 0.2
epsilon = 1e-06
f32 = jnp.float32
bf16 = jnp.bfloat16


def shift(value, axis, by):
    size = lax.axis_size(axis)
    return lax.ppermute(value, axis, [(i, (i + by) % size) for i in range(size)])


def ring_gather(value, axis, put, result, half_dim):
    size, me = lax.axis_size(axis), lax.axis_index(axis)
    result = put(result, value, me, 0)
    up = down = value
    for step in range(1, size // 2):
        up, down = shift(up, axis, 1), shift(down, axis, -1)
        result = put(result, up, (me - step + size) % size, 0)
        result = put(result, down, (me + step) % size, 0)
    half = value.shape[half_dim] // 2
    first = lax.slice_in_dim(up, 0, half, axis=half_dim)
    second = lax.slice_in_dim(down, half, 2 * half, axis=half_dim)
    opposite = (me + size // 2) % size
    result = put(result, shift(first, axis, 1), opposite, 0)
    return put(result, shift(second, axis, -1), opposite, half)


def gather_plane(value, first, second):
    n_0, n_1 = (lax.axis_size(axis) for axis in PLANE)

    def put_line(line, block, owner, row):
        return lax.dynamic_update_slice(line, block[None], (owner, row, 0))

    def put_plane(plane, block, owner, begin):
        if second == PLANE[0]:
            return lax.dynamic_update_slice(plane, block[None], (owner, begin, 0, 0))
        return lax.dynamic_update_slice(plane, block[:, None], (begin, owner, 0, 0))

    line = jnp.zeros((lax.axis_size(first), *value.shape), value.dtype)
    size, me = lax.axis_size(first), lax.axis_index(first)
    line = put_line(line, value, me, 0)
    for by in (1, -1, 2):
        line = put_line(line, shift(value, first, by), (me - by + size) % size, 0)
    plane = jnp.zeros((n_0, n_1, *value.shape), value.dtype)
    return ring_gather(line, second, put_plane, plane, 0)


def from_everyone(value, axes):
    size = lax.axis_size(axes)
    copies = jnp.broadcast_to(value[None], (size, *value.shape))
    return lax.all_to_all(copies, axes, 0, 0, tiled=True)


def dot(left, right, left_dim, right_dim):
    return lax.dot_general(
        left, right, (((left_dim,), (right_dim,)), ((), ())), preferred_element_type=f32
    )


def split(value):
    high = lax.reduce_precision(value, 8, 7)
    middle = lax.reduce_precision(value - high, 8, 7)
    return [t.astype(bf16) for t in (high, middle, value - high - middle)]


def whitened_kernel(core_ref, scale_ref, both_ref, q_ref, q_other_ref, inv_ref, inv_other_ref, out_ref, sums):
    step = pl.program_id(0)
    rows, columns = out_ref.shape[0] // 2, out_ref.shape[1] // 2

    @pl.when(step == 0)
    def _():
        sums[...] = jnp.zeros_like(sums)

    for i, refs in enumerate(((q_ref, q_other_ref), (inv_ref, inv_other_ref))):
        values = both_ref[i * rows : (i + 1) * rows, :]
        for j, ref in enumerate(refs):
            sums[j, i * rows : (i + 1) * rows, :] += jnp.dot(
                values, ref[...], preferred_element_type=f32
            )

    @pl.when(step == pl.num_programs(0) - 1)
    def _():
        mine, others = (scale_ref[...] * sums[j] for j in range(2))
        first = core_ref[0] == 0
        out_ref[:, :columns] = jnp.where(first, mine, others).astype(out_ref.dtype)
        out_ref[:, columns:] = jnp.where(first, others, mine).astype(out_ref.dtype)


def whitened(core, scale, both, *factors):
    (rows, depth), half = both.shape, factors[0].shape[1]
    deep = min(512, depth)
    return pl.pallas_call(
        whitened_kernel,
        grid=(depth // deep,),
        out_shape=jax.ShapeDtypeStruct((rows, 2 * half), bf16),
        in_specs=[
            pl.BlockSpec(memory_space=pltpu.SMEM),
            pl.BlockSpec((rows, 1), lambda k: (0, 0)),
            pl.BlockSpec((rows, deep), lambda k: (0, k)),
            *[pl.BlockSpec((deep, half), lambda k: (k, 0)) for _ in factors],
        ],
        out_specs=pl.BlockSpec((rows, 2 * half), lambda k: (0, 0)),
        scratch_shapes=[pltpu.VMEM((2, rows, half), f32)],
        cost_estimate=pl.CostEstimate(
            flops=4 * rows * depth * half, bytes_accessed=2 * depth * (rows + 4 * half), transcendentals=0
        ),
        name="whitened",
    )(core[None], scale, both, *factors)


def body(grads, probe, left_factor, q_right, q_inv_t):
    n_cols, me = lax.axis_size(COLS), lax.axis_index(COLS)
    core = lax.axis_index(CORE)
    n_plane = lax.axis_size(PLANE)
    height, width = grads.shape
    half = width // 2
    piece = half // n_plane

    q_low = q_right.astype(bf16)
    inv_low = q_inv_t.astype(bf16)
    both = lax.all_gather(jnp.concatenate([grads, probe], axis=0), COLS, axis=1, tiled=True)

    def half_of(value, which):
        return lax.dynamic_slice_in_dim(value, which * half, half, axis=1)

    def in_core_order(mine, others, axis):
        first = jnp.concatenate([mine, others], axis=axis)
        second = jnp.concatenate([others, mine], axis=axis)
        return jnp.where(core == 0, first, second)

    q_t, inv_t = q_low.T, inv_low.T
    got = shift(jnp.concatenate([half_of(q_t, 1 - core), half_of(inv_t, 1 - core)], axis=1), CORE, 1)
    q_pair = in_core_order(half_of(q_t, core), got[:, :half], 0)
    inv_pair = in_core_order(half_of(inv_t, core), got[:, half:], 0)
    q_half = gather_plane(q_pair, "rows_1", "rows_0").reshape(-1, half)
    inv_half = gather_plane(inv_pair, "rows_0", "rows_1").reshape(-1, half)
    q_other, inv_other = shift(q_half, CORE, 1), shift(inv_half, CORE, 1)

    scale = jnp.concatenate([left_factor, 1.0 / left_factor])[:, None]
    own = whitened(core, scale, both, q_half, q_other, inv_half, inv_other)
    white, conj = own[:height], own[height:]

    before = shift(own, COLS, 1)
    behind = shift(own, COLS, -1)
    before_2 = shift(before, COLS, 1)
    behind_2 = shift(behind, COLS, -1)

    def pair(left, right):
        signed = jnp.concatenate([right[:height], -right[height:]], axis=0)
        return with_layout_constraint(dot(left, signed, 0, 0), Layout(major_to_minor=(0, 1)))

    def over_cores(pairs):
        products = []
        for a, b in pairs:
            products.append(pair(a, b))
        part = jnp.concatenate(products, axis=1)
        keep = lax.dynamic_slice_in_dim(part, core * half, half, axis=0)
        give = lax.dynamic_slice_in_dim(part, (1 - core) * half, half, axis=0).astype(bf16)
        got = shift(give, CORE, 1)
        part = (keep + got.astype(f32)).astype(bf16)
        return part.reshape(n_plane, piece, part.shape[1])

    def over_plane(part):
        parts = lax.all_to_all(part, PLANE, 0, 0, tiled=True)
        return jnp.sum(parts.astype(f32), axis=0)

    early_part = over_cores([(own, own), (own, behind)])
    early = over_plane(early_part)
    white_f, conj_f = white.astype(f32), conj.astype(f32)
    left_part = jnp.sum(white_f * white_f - conj_f * conj_f, axis=1)
    strip = q_low.shape[1]
    lines = height // strip
    terms = jnp.stack(split(left_part)).reshape(3 * lines, strip)
    terms = jnp.pad(terms, ((0, 16 - 3 * lines), (0, 0)))
    q_all = lax.all_gather(jnp.concatenate([q_low, terms], axis=0), COLS, axis=0, tiled=True)
    q_all = q_all.reshape(n_cols, width + 16, -1)
    terms = q_all[:, width : width + 3 * lines].astype(f32).reshape(n_cols, 3, height)
    left_grad = jnp.sum((terms[:, 0] + terms[:, 1]) + terms[:, 2], axis=0)
    top_l = jnp.max(jnp.abs(left_grad))
    before_2, behind_2, _ = lax.optimization_barrier((before_2, behind_2, early_part))
    late_part = over_cores([(before, behind), (before, behind_2), (before_2, behind_2)])
    late = over_plane(late_part)


    top_r = jnp.maximum(jnp.max(jnp.abs(early)), jnp.max(jnp.abs(late)))
    terms = jnp.stack(split(jnp.stack([top_r, top_l]))).reshape(1, 6)
    note = jnp.broadcast_to(jnp.pad(terms, ((0, 0), (0, 122))), (piece, 128))
    pieces = jnp.concatenate([early.astype(bf16), late.astype(bf16), note], axis=1)
    mine = from_everyone(pieces, PLANE).reshape(half, -1)
    gram = in_core_order(mine, shift(mine, CORE, 1), 0)

    def joined(terms):
        terms = terms.astype(f32)
        return (terms[:, 0] + terms[:, 1]) + terms[:, 2]

    top_r, top_l = jnp.max(joined(gram[:, 5 * width : 5 * width + 6].reshape(width, 3, 2)), axis=0)
    top_r = jnp.full((8, 128), top_r)
    top_r = jnp.maximum(top_r, shift(top_r, COLS, n_cols // 2))[0, 0]

    def block(i, size=1):
        return gram[:, i * width : (i + size) * width]

    def q_at(by, size=1):
        rows = [
            lax.dynamic_index_in_dim(q_all, (me + by + i + n_cols) % n_cols, 0, keepdims=False)[:width]
            for i in range(size)
        ]
        return jnp.concatenate(rows, axis=0)

    note = jnp.pad(jnp.stack(split(top_r))[:, None], ((0, 13), (0, strip - 1)))

    def sent(value, by):
        return shift(jnp.concatenate([value.astype(bf16), note], axis=0), COLS, by)

    got = [
        sent(dot(block(4), q_at(2), 1, 0), -2),
        sent(dot(block(3), q_at(-1), 0, 0), 2),
        sent(dot(block(2, 2), q_at(1, 2), 1, 0), -1),
        sent(dot(block(1), q_at(0), 0, 0) + dot(block(2), q_at(-1), 0, 0), 1),
    ]
    product = dot(block(0, 2), q_at(0, 2), 1, 0)
    for value in got:
        product = product + value[:width].astype(f32)
        top_r = jnp.maximum(top_r, joined(value[width : width + 3, :1].T)[0])
    scale_r = learn_rate / (top_r + epsilon)
    scale_l = learn_rate / (top_l + epsilon)
    left_new = left_factor - scale_l * left_grad * left_factor
    q_new = q_right - scale_r * product
    return (left_new, q_new)


def solution(mesh):
    finer = Mesh(
        mesh.devices.reshape(4, 4, 2, mesh.shape["cols"]), ("rows_0", "rows_1", "rows_2", "cols")
    )
    in_specs = (P(ROWS, "cols"), P(ROWS, "cols"), P(ROWS), P("cols", ROWS), P("cols", ROWS))
    out_specs = (P(ROWS), P("cols", ROWS))

    return jax.shard_map(body, mesh=finer, in_specs=in_specs, out_specs=out_specs, check_vma=False)
```

```python
import jax
import jax.numpy as jnp
from jax import lax
from jax.experimental import pallas as pl
from jax.experimental.layout import Layout, with_layout_constraint
from jax.experimental.pallas import tpu as pltpu
from jax.sharding import Mesh
from jax.sharding import PartitionSpec as P

ROWS = ("rows_0", "rows_1", "rows_2")
PLANE = ("rows_0", "rows_1")
CORE = "rows_2"
COLS = "cols"


learn_rate = 0.2
epsilon = 1e-06
f32 = jnp.float32
bf16 = jnp.bfloat16


def shift(value, axis, by):
    size = lax.axis_size(axis)
    return lax.ppermute(value, axis, [(i, (i + by) % size) for i in range(size)])


def ring_gather(value, axis, put, result, half_dim):
    size, me = lax.axis_size(axis), lax.axis_index(axis)
    result = put(result, value, me, 0)
    up = down = value
    for step in range(1, size // 2):
        up, down = shift(up, axis, 1), shift(down, axis, -1)
        result = put(result, up, (me - step + size) % size, 0)
        result = put(result, down, (me + step) % size, 0)
    half = value.shape[half_dim] // 2
    first = lax.slice_in_dim(up, 0, half, axis=half_dim)
    second = lax.slice_in_dim(down, half, 2 * half, axis=half_dim)
    opposite = (me + size // 2) % size
    result = put(result, shift(first, axis, 1), opposite, 0)
    return put(result, shift(second, axis, -1), opposite, half)


def gather_plane(value, first, second):
    n_0, n_1 = (lax.axis_size(axis) for axis in PLANE)

    def put_line(line, block, owner, row):
        return lax.dynamic_update_slice(line, block[None], (owner, row, 0))

    def put_plane(plane, block, owner, begin):
        if second == PLANE[0]:
            return lax.dynamic_update_slice(plane, block[None], (owner, begin, 0, 0))
        return lax.dynamic_update_slice(plane, block[:, None], (begin, owner, 0, 0))

    line = jnp.zeros((lax.axis_size(first), *value.shape), value.dtype)
    size, me = lax.axis_size(first), lax.axis_index(first)
    line = put_line(line, value, me, 0)
    for by in (1, -1, 2):
        line = put_line(line, shift(value, first, by), (me - by + size) % size, 0)
    plane = jnp.zeros((n_0, n_1, *value.shape), value.dtype)
    return ring_gather(line, second, put_plane, plane, 0)


def from_everyone(value, axes):
    size = lax.axis_size(axes)
    copies = jnp.broadcast_to(value[None], (size, *value.shape))
    return lax.all_to_all(copies, axes, 0, 0, tiled=True)


def dot(left, right, left_dim, right_dim):
    return lax.dot_general(
        left, right, (((left_dim,), (right_dim,)), ((), ())), preferred_element_type=f32
    )


def whitened_kernel(core_ref, scale_ref, more_ref, both_ref, q_ref, q_other_ref, inv_ref, inv_other_ref, out_ref, sums):
    step = pl.program_id(0)
    rows, columns = both_ref.shape[0] // 2, out_ref.shape[1] // 2

    @pl.when(step == 0)
    def _():
        sums[...] = jnp.zeros_like(sums)

    for i, refs in enumerate(((q_ref, q_other_ref), (inv_ref, inv_other_ref))):
        values = both_ref[i * rows : (i + 1) * rows, :]
        for j, ref in enumerate(refs):
            sums[j, i * rows : (i + 1) * rows, :] += jnp.dot(
                values, ref[...], preferred_element_type=f32
            )

    @pl.when(step == pl.num_programs(0) - 1)
    def _():
        mine, others = (scale_ref[...] * sums[j] for j in range(2))
        first = core_ref[0] == 0
        out_ref[: 2 * rows, :columns] = jnp.where(first, mine, others).astype(out_ref.dtype)
        out_ref[: 2 * rows, columns:] = jnp.where(first, others, mine).astype(out_ref.dtype)
        out_ref[2 * rows :, :] = more_ref[...]


def whitened(core, scale, more, both, *factors):
    (rows, depth), half = both.shape, factors[0].shape[1]
    deep = min(512, depth)
    return pl.pallas_call(
        whitened_kernel,
        grid=(depth // deep,),
        out_shape=jax.ShapeDtypeStruct((rows + more.shape[0], 2 * half), bf16),
        in_specs=[
            pl.BlockSpec(memory_space=pltpu.SMEM),
            pl.BlockSpec((rows, 1), lambda k: (0, 0)),
            pl.BlockSpec(more.shape, lambda k: (0, 0)),
            pl.BlockSpec((rows, deep), lambda k: (0, k)),
            *[pl.BlockSpec((deep, half), lambda k: (k, 0)) for _ in factors],
        ],
        out_specs=pl.BlockSpec((rows + more.shape[0], 2 * half), lambda k: (0, 0)),
        scratch_shapes=[pltpu.VMEM((2, rows, half), f32)],
        cost_estimate=pl.CostEstimate(
            flops=4 * rows * depth * half, bytes_accessed=2 * depth * (rows + 4 * half), transcendentals=0
        ),
        name="whitened",
    )(core[None], scale, more, both, *factors)


def body(grads, probe, left_factor, q_right, q_inv_t):
    core = lax.axis_index(CORE)
    n_plane = lax.axis_size(PLANE)
    height, width = grads.shape
    half = width // 2
    piece = half // n_plane

    q_low = q_right.astype(bf16)
    inv_low = q_inv_t.astype(bf16)
    both = lax.all_gather(jnp.concatenate([grads, probe], axis=0), COLS, axis=1, tiled=True)

    def half_of(value, which):
        return lax.dynamic_slice_in_dim(value, which * half, half, axis=1)

    def in_core_order(mine, others, axis):
        first = jnp.concatenate([mine, others], axis=axis)
        second = jnp.concatenate([others, mine], axis=axis)
        return jnp.where(core == 0, first, second)

    q_t, inv_t = q_low.T, inv_low.T
    got = shift(jnp.concatenate([half_of(q_t, 1 - core), half_of(inv_t, 1 - core)], axis=1), CORE, 1)
    q_pair = in_core_order(half_of(q_t, core), got[:, :half], 0)
    inv_pair = in_core_order(half_of(inv_t, core), got[:, half:], 0)
    q_half = gather_plane(q_pair, "rows_1", "rows_0").reshape(-1, half)
    inv_half = gather_plane(inv_pair, "rows_0", "rows_1").reshape(-1, half)
    q_other, inv_other = shift(q_half, CORE, 1), shift(inv_half, CORE, 1)

    scale = jnp.concatenate([left_factor, 1.0 / left_factor])[:, None]
    own = whitened(core, scale, q_t, both, q_half, q_other, inv_half, inv_other)
    white, conj = own[:height], own[height : 2 * height]

    before = shift(own, COLS, 1)
    behind = shift(own, COLS, -1)
    before_2 = shift(before, COLS, 1)
    behind_2 = shift(behind, COLS, -1)

    def pair(left, right):
        signed = jnp.concatenate([right[:height], -right[height : 2 * height]], axis=0)
        return with_layout_constraint(dot(left[: 2 * height], signed, 0, 0), Layout(major_to_minor=(0, 1)))

    def over_cores(pairs):
        products = []
        for a, b in pairs:
            products.append(pair(a, b))
        part = jnp.concatenate(products, axis=1)
        keep = lax.dynamic_slice_in_dim(part, core * half, half, axis=0)
        give = lax.dynamic_slice_in_dim(part, (1 - core) * half, half, axis=0).astype(bf16)
        got = shift(give, CORE, 1)
        part = (keep + got.astype(f32)).astype(bf16)
        return part.reshape(n_plane, piece, part.shape[1])

    def over_plane(part):
        parts = lax.all_to_all(part, PLANE, 0, 0, tiled=True)
        return jnp.sum(parts.astype(f32), axis=0)

    early_part = over_cores([(own, own), (own, behind)])
    early = over_plane(early_part)
    white_f, conj_f = white.astype(f32), conj.astype(f32)
    left_part = jnp.sum(white_f * white_f - conj_f * conj_f, axis=1)
    left_parts = from_everyone(left_part.reshape(-1, 128), COLS)
    left_grad = jnp.sum(left_parts, axis=0).reshape(height)
    top_l = jnp.max(jnp.abs(left_grad))
    before_2, behind_2, _ = lax.optimization_barrier((before_2, behind_2, early_part))
    late_part = over_cores([(before, behind), (before, behind_2), (before_2, behind_2)])
    late = over_plane(late_part)


    top_r = jnp.maximum(jnp.max(jnp.abs(early)), jnp.max(jnp.abs(late)))
    line = lax.broadcasted_iota(jnp.int32, (8, 128), 0)
    tops = lax.optimization_barrier(jnp.where(line == 0, top_r, top_l))
    tops = lax.all_gather(tops, (*ROWS, COLS), axis=0)
    tops = jnp.max(tops, axis=0)
    scale_r, scale_l = (learn_rate / (tops[i, 0] + epsilon) for i in range(2))

    pieces = jnp.concatenate([early.astype(bf16), late.astype(bf16)], axis=1)
    mine = from_everyone(pieces, PLANE).reshape(half, -1)
    gram = in_core_order(mine, shift(mine, CORE, 1), 0)

    def block(i, size=1):
        return gram[:, i * width : (i + size) * width]

    q_near = {i: v[2 * height :] for i, v in ((-1, before), (0, own), (1, behind), (2, behind_2))}

    def times(i, by):
        value, q = block(i, len(by)), jnp.concatenate([q_near[j] for j in by], axis=1)
        return dot(value, q, 1, 1)

    def turned_times(i, by):
        return dot(block(i), q_near[by], 0, 1)

    def sent(value, by):
        return shift(value.astype(bf16), COLS, by).astype(f32)

    got = [
        sent(times(4, (2,)), -2),
        sent(turned_times(3, -1), 2),
        sent(times(2, (1, 2)), -1),
        sent(turned_times(1, 0) + turned_times(2, -1), 1),
    ]
    product = times(0, (0, 1)) + ((got[0] + got[1]) + (got[2] + got[3]))
    left_new = left_factor - scale_l * left_grad * left_factor
    q_new = q_right - scale_r * product
    return (left_new, q_new)


def solution(mesh):
    finer = Mesh(
        mesh.devices.reshape(4, 4, 2, mesh.shape["cols"]), ("rows_0", "rows_1", "rows_2", "cols")
    )
    in_specs = (P(ROWS, "cols"), P(ROWS, "cols"), P(ROWS), P("cols", ROWS), P("cols", ROWS))
    out_specs = (P(ROWS), P("cols", ROWS))

    return jax.shard_map(body, mesh=finer, in_specs=in_specs, out_specs=out_specs, check_vma=False)
```

```python
import jax
import jax.numpy as jnp
from jax import lax
from jax.experimental import pallas as pl
from jax.experimental.layout import Layout, with_layout_constraint
from jax.experimental.pallas import tpu as pltpu
from jax.sharding import Mesh
from jax.sharding import PartitionSpec as P

ROWS = ("rows_0", "rows_1", "rows_2")
PLANE = ("rows_0", "rows_1")
CORE = "rows_2"
COLS = "cols"


learn_rate = 0.2
epsilon = 1e-06
f32 = jnp.float32
bf16 = jnp.bfloat16


def shift(value, axis, by):
    size = lax.axis_size(axis)
    return lax.ppermute(value, axis, [(i, (i + by) % size) for i in range(size)])


def ring_gather(value, axis, put, result, half_dim):
    size, me = lax.axis_size(axis), lax.axis_index(axis)
    result = put(result, value, me, 0)
    up = down = value
    for step in range(1, size // 2):
        up, down = shift(up, axis, 1), shift(down, axis, -1)
        result = put(result, up, (me - step + size) % size, 0)
        result = put(result, down, (me + step) % size, 0)
    half = value.shape[half_dim] // 2
    first = lax.slice_in_dim(up, 0, half, axis=half_dim)
    second = lax.slice_in_dim(down, half, 2 * half, axis=half_dim)
    opposite = (me + size // 2) % size
    result = put(result, shift(first, axis, 1), opposite, 0)
    return put(result, shift(second, axis, -1), opposite, half)


def gather_plane(value, first, second):
    n_0, n_1 = (lax.axis_size(axis) for axis in PLANE)

    def put_line(line, block, owner, row):
        return lax.dynamic_update_slice(line, block[None], (owner, row, 0))

    def put_plane(plane, block, owner, begin):
        if second == PLANE[0]:
            return lax.dynamic_update_slice(plane, block[None], (owner, begin, 0, 0))
        return lax.dynamic_update_slice(plane, block[:, None], (begin, owner, 0, 0))

    line = jnp.zeros((lax.axis_size(first), *value.shape), value.dtype)
    size, me = lax.axis_size(first), lax.axis_index(first)
    line = put_line(line, value, me, 0)
    for by in (1, -1, 2):
        line = put_line(line, shift(value, first, by), (me - by + size) % size, 0)
    plane = jnp.zeros((n_0, n_1, *value.shape), value.dtype)
    return ring_gather(line, second, put_plane, plane, 0)


def from_everyone(value, axes):
    size = lax.axis_size(axes)
    copies = jnp.broadcast_to(value[None], (size, *value.shape))
    return lax.all_to_all(copies, axes, 0, 0, tiled=True)


def dot(left, right, left_dim, right_dim):
    return lax.dot_general(
        left, right, (((left_dim,), (right_dim,)), ((), ())), preferred_element_type=f32
    )


def after(values, *others):
    return lax.optimization_barrier((values, *others))[0]


def split(value):
    high = lax.reduce_precision(value, 8, 7)
    middle = lax.reduce_precision(value - high, 8, 7)
    return high, middle, value - high - middle


def whitened_kernel(core_ref, scale_ref, both_ref, q_ref, q_other_ref, inv_ref, inv_other_ref, out_ref, sums):
    step = pl.program_id(0)
    rows, columns = out_ref.shape[0] // 2, out_ref.shape[1] // 2

    @pl.when(step == 0)
    def _():
        sums[...] = jnp.zeros_like(sums)

    for i, refs in enumerate(((q_ref, q_other_ref), (inv_ref, inv_other_ref))):
        values = both_ref[i * rows : (i + 1) * rows, :]
        for j, ref in enumerate(refs):
            sums[j, i * rows : (i + 1) * rows, :] += jnp.dot(
                values, ref[...], preferred_element_type=f32
            )

    @pl.when(step == pl.num_programs(0) - 1)
    def _():
        mine, others = (scale_ref[...] * sums[j] for j in range(2))
        first = core_ref[0] == 0
        out_ref[:, :columns] = jnp.where(first, mine, others).astype(out_ref.dtype)
        out_ref[:, columns:] = jnp.where(first, others, mine).astype(out_ref.dtype)


def whitened(core, scale, both, *factors):
    (rows, depth), half = both.shape, factors[0].shape[1]
    deep = min(512, depth)
    return pl.pallas_call(
        whitened_kernel,
        grid=(depth // deep,),
        out_shape=jax.ShapeDtypeStruct((rows, 2 * half), bf16),
        in_specs=[
            pl.BlockSpec(memory_space=pltpu.SMEM),
            pl.BlockSpec((rows, 1), lambda k: (0, 0)),
            pl.BlockSpec((rows, deep), lambda k: (0, k)),
            *[pl.BlockSpec((deep, half), lambda k: (k, 0)) for _ in factors],
        ],
        out_specs=pl.BlockSpec((rows, 2 * half), lambda k: (0, 0)),
        scratch_shapes=[pltpu.VMEM((2, rows, half), f32)],
        cost_estimate=pl.CostEstimate(
            flops=4 * rows * depth * half, bytes_accessed=2 * depth * (rows + 4 * half), transcendentals=0
        ),
        name="whitened",
    )(core[None], scale, both, *factors)


def body(grads, probe, left_factor, q_right, q_inv_t):
    n_cols, me = lax.axis_size(COLS), lax.axis_index(COLS)
    core = lax.axis_index(CORE)
    n_plane = lax.axis_size(PLANE)
    height, width = grads.shape
    half = width // 2
    piece = half // n_plane

    q_low = q_right.astype(bf16)
    inv_low = q_inv_t.astype(bf16)
    both = lax.all_gather(jnp.concatenate([grads, probe], axis=0), COLS, axis=1, tiled=True)

    def half_of(value, which):
        return lax.dynamic_slice_in_dim(value, which * half, half, axis=1)

    def in_core_order(mine, others, axis):
        first = jnp.concatenate([mine, others], axis=axis)
        second = jnp.concatenate([others, mine], axis=axis)
        return jnp.where(core == 0, first, second)

    q_t, inv_t = q_low.T, inv_low.T
    got = shift(jnp.concatenate([half_of(q_t, 1 - core), half_of(inv_t, 1 - core)], axis=1), CORE, 1)
    q_pair = in_core_order(half_of(q_t, core), got[:, :half], 0)
    inv_pair = in_core_order(half_of(inv_t, core), got[:, half:], 0)
    q_half = gather_plane(q_pair, "rows_1", "rows_0").reshape(-1, half)
    inv_half = gather_plane(inv_pair, "rows_0", "rows_1").reshape(-1, half)
    q_other, inv_other = shift(q_half, CORE, 1), shift(inv_half, CORE, 1)

    scale = jnp.concatenate([left_factor, 1.0 / left_factor])[:, None]
    own = whitened(core, scale, both, q_half, q_other, inv_half, inv_other)
    white, conj = own[:height], own[height:]

    before = shift(own, COLS, 1)
    behind = shift(own, COLS, -1)
    before_2 = shift(before, COLS, 1)
    behind_2 = shift(behind, COLS, -1)

    def pair(left, right):
        signed = jnp.concatenate([right[:height], -right[height:]], axis=0)
        return with_layout_constraint(dot(left, signed, 0, 0), Layout(major_to_minor=(0, 1)))

    def over_cores(pairs):
        products = []
        for a, b in pairs:
            products.append(pair(a, b))
        part = jnp.concatenate(products, axis=1)
        keep = lax.dynamic_slice_in_dim(part, core * half, half, axis=0)
        give = lax.dynamic_slice_in_dim(part, (1 - core) * half, half, axis=0).astype(bf16)
        got = shift(give, CORE, 1)
        part = (keep + got.astype(f32)).astype(bf16)
        return part.reshape(n_plane, piece, part.shape[1])

    def over_plane(part):
        parts = lax.all_to_all(part, PLANE, 0, 0, tiled=True)
        return jnp.sum(parts.astype(f32), axis=0)

    early_part = over_cores([(own, own), (own, behind)])
    early = over_plane(early_part)
    white_f, conj_f = white.astype(f32), conj.astype(f32)
    left_part = jnp.sum(white_f * white_f - conj_f * conj_f, axis=1)
    left_parts = from_everyone(left_part.reshape(-1, 128), COLS)
    left_grad = jnp.sum(left_parts, axis=0).reshape(height)
    top_l = jnp.max(jnp.abs(left_grad))
    before_2, behind_2, _ = lax.optimization_barrier((before_2, behind_2, early_part))
    late_part = over_cores([(before, behind), (before, behind_2), (before_2, behind_2)])
    late = over_plane(late_part)


    q_all = lax.all_gather(after(q_low, late_part), COLS, axis=0)

    top_r = jnp.maximum(jnp.max(jnp.abs(early)), jnp.max(jnp.abs(late)))
    lane = lax.broadcasted_iota(jnp.int32, (piece, 128), 1)
    terms = split(jnp.where(lane < 3, top_r, top_l))
    note = jnp.where(lane % 3 == 0, terms[0], jnp.where(lane % 3 == 1, terms[1], terms[2]))
    pieces = jnp.concatenate([early.astype(bf16), late.astype(bf16), note.astype(bf16)], axis=1)
    mine = from_everyone(pieces, PLANE)
    notes = mine[:, :1, 5 * width :].astype(f32)
    lane = lax.broadcasted_iota(jnp.int32, notes.shape, 2)
    tops = [
        jnp.max(jnp.sum(jnp.where((lane >= i) & (lane < i + 3), notes, 0.0), axis=2, keepdims=True), axis=0)
        for i in (0, 3)
    ]
    lane = lax.broadcasted_iota(jnp.int32, (8, 128), 1)
    tops = from_everyone(jnp.where(lane == 0, *tops), (CORE, COLS))
    mine = mine[:, :, : 5 * width].reshape(half, -1)
    gram = in_core_order(mine, shift(mine, CORE, 1), 0)

    def block(i, size=1):
        return gram[:, i * width : (i + size) * width]

    def times(i, by):
        rows = [lax.dynamic_index_in_dim(q_all, (me + j + n_cols) % n_cols, 0, keepdims=False) for j in by]
        return dot(block(i, len(by)), jnp.concatenate(rows, axis=0), 1, 0)

    def turned_times(i, by):
        rows = lax.dynamic_index_in_dim(q_all, (me + by + n_cols) % n_cols, 0, keepdims=False)
        return dot(block(i), rows, 0, 0)

    def sent(value, by):
        return shift(value.astype(bf16), COLS, by).astype(f32)

    values = [turned_times(3, -1), times(4, (2,)), times(2, (1, 2)), turned_times(1, 0) + turned_times(2, -1)]
    got = [sent(value, by) for value, by in zip(values, (2, -2, -1, 1), strict=True)]
    product = times(0, (0, 1))
    tops = jnp.max(after(tops, values[3], product), axis=(0, 1))
    scale_r, scale_l = (learn_rate / (tops[i] + epsilon) for i in range(2))
    product = product + ((got[0] + got[1]) + (got[2] + got[3]))
    left_new = left_factor - scale_l * left_grad * left_factor
    q_new = q_right - scale_r * product
    return (left_new, q_new)


def solution(mesh):
    finer = Mesh(
        mesh.devices.reshape(4, 4, 2, mesh.shape["cols"]), ("rows_0", "rows_1", "rows_2", "cols")
    )
    in_specs = (P(ROWS, "cols"), P(ROWS, "cols"), P(ROWS), P("cols", ROWS), P("cols", ROWS))
    out_specs = (P(ROWS), P("cols", ROWS))

    return jax.shard_map(body, mesh=finer, in_specs=in_specs, out_specs=out_specs, check_vma=False)
```

```python
import jax
import jax.numpy as jnp
from jax import lax
from jax.experimental import pallas as pl
from jax.experimental.layout import Layout, with_layout_constraint
from jax.experimental.pallas import tpu as pltpu
from jax.sharding import Mesh
from jax.sharding import PartitionSpec as P

ROWS = ("rows_0", "rows_1", "rows_2")
PLANE = ("rows_0", "rows_1")
CORE = "rows_2"
COLS = "cols"


learn_rate = 0.2
epsilon = 1e-06
f32 = jnp.float32
bf16 = jnp.bfloat16


def shift(value, axis, by):
    size = lax.axis_size(axis)
    return lax.ppermute(value, axis, [(i, (i + by) % size) for i in range(size)])


def ring_gather(value, axis, put, result, half_dim):
    size, me = lax.axis_size(axis), lax.axis_index(axis)
    result = put(result, value, me, 0)
    up = down = value
    for step in range(1, size // 2):
        up, down = shift(up, axis, 1), shift(down, axis, -1)
        result = put(result, up, (me - step + size) % size, 0)
        result = put(result, down, (me + step) % size, 0)
    half = value.shape[half_dim] // 2
    first = lax.slice_in_dim(up, 0, half, axis=half_dim)
    second = lax.slice_in_dim(down, half, 2 * half, axis=half_dim)
    opposite = (me + size // 2) % size
    result = put(result, shift(first, axis, 1), opposite, 0)
    return put(result, shift(second, axis, -1), opposite, half)


def gather_plane(value, first, second):
    n_0, n_1 = (lax.axis_size(axis) for axis in PLANE)

    def put_line(line, block, owner, row):
        return lax.dynamic_update_slice(line, block[None], (owner, row, 0))

    def put_plane(plane, block, owner, begin):
        if second == PLANE[0]:
            return lax.dynamic_update_slice(plane, block[None], (owner, begin, 0, 0))
        return lax.dynamic_update_slice(plane, block[:, None], (begin, owner, 0, 0))

    line = jnp.zeros((lax.axis_size(first), *value.shape), value.dtype)
    size, me = lax.axis_size(first), lax.axis_index(first)
    line = put_line(line, value, me, 0)
    for by in (1, -1, 2):
        line = put_line(line, shift(value, first, by), (me - by + size) % size, 0)
    plane = jnp.zeros((n_0, n_1, *value.shape), value.dtype)
    return ring_gather(line, second, put_plane, plane, 0)


def from_everyone(value, axes):
    size = lax.axis_size(axes)
    copies = jnp.broadcast_to(value[None], (size, *value.shape))
    return lax.all_to_all(copies, axes, 0, 0, tiled=True)


def dot(left, right, left_dim, right_dim):
    return lax.dot_general(
        left, right, (((left_dim,), (right_dim,)), ((), ())), preferred_element_type=f32
    )


def after(values, *others):
    return lax.optimization_barrier((values, *others))[0]


def split(value):
    high = lax.reduce_precision(value, 8, 7)
    middle = lax.reduce_precision(value - high, 8, 7)
    return high, middle, value - high - middle


def whitened_kernel(core_ref, scale_ref, both_ref, q_ref, q_other_ref, inv_ref, inv_other_ref, out_ref, sums):
    step = pl.program_id(0)
    rows, columns = out_ref.shape[0] // 2, out_ref.shape[1] // 2

    @pl.when(step == 0)
    def _():
        sums[...] = jnp.zeros_like(sums)

    for i, refs in enumerate(((q_ref, q_other_ref), (inv_ref, inv_other_ref))):
        values = both_ref[i * rows : (i + 1) * rows, :]
        for j, ref in enumerate(refs):
            sums[j, i * rows : (i + 1) * rows, :] += jnp.dot(
                values, ref[...], preferred_element_type=f32
            )

    @pl.when(step == pl.num_programs(0) - 1)
    def _():
        mine, others = (scale_ref[...] * sums[j] for j in range(2))
        first = core_ref[0] == 0
        out_ref[:, :columns] = jnp.where(first, mine, others).astype(out_ref.dtype)
        out_ref[:, columns:] = jnp.where(first, others, mine).astype(out_ref.dtype)


def whitened(core, scale, both, *factors):
    (rows, depth), half = both.shape, factors[0].shape[1]
    deep = min(1024, depth)
    return pl.pallas_call(
        whitened_kernel,
        grid=(depth // deep,),
        out_shape=jax.ShapeDtypeStruct((rows, 2 * half), bf16),
        in_specs=[
            pl.BlockSpec(memory_space=pltpu.SMEM),
            pl.BlockSpec((rows, 1), lambda k: (0, 0)),
            pl.BlockSpec((rows, deep), lambda k: (0, k)),
            *[pl.BlockSpec((deep, half), lambda k: (k, 0)) for _ in factors],
        ],
        out_specs=pl.BlockSpec((rows, 2 * half), lambda k: (0, 0)),
        scratch_shapes=[pltpu.VMEM((2, rows, half), f32)],
        compiler_params=pltpu.CompilerParams(vmem_limit_bytes=16 * 2**20),
        cost_estimate=pl.CostEstimate(
            flops=4 * rows * depth * half, bytes_accessed=2 * depth * (rows + 4 * half), transcendentals=0
        ),
        name="whitened",
    )(core[None], scale, both, *factors)


def body(grads, probe, left_factor, q_right, q_inv_t):
    n_cols, me = lax.axis_size(COLS), lax.axis_index(COLS)
    core = lax.axis_index(CORE)
    n_plane = lax.axis_size(PLANE)
    height, width = grads.shape
    half = width // 2
    piece = half // n_plane

    q_low = q_right.astype(bf16)
    inv_low = q_inv_t.astype(bf16)
    both = lax.all_gather(jnp.concatenate([grads, probe], axis=0), COLS, axis=1, tiled=True)

    def half_of(value, which):
        return lax.dynamic_slice_in_dim(value, which * half, half, axis=1)

    def in_core_order(mine, others, axis):
        first = jnp.concatenate([mine, others], axis=axis)
        second = jnp.concatenate([others, mine], axis=axis)
        return jnp.where(core == 0, first, second)

    q_t, inv_t = q_low.T, inv_low.T
    got = shift(jnp.concatenate([half_of(q_t, 1 - core), half_of(inv_t, 1 - core)], axis=1), CORE, 1)
    q_pair = in_core_order(half_of(q_t, core), got[:, :half], 0)
    inv_pair = in_core_order(half_of(inv_t, core), got[:, half:], 0)
    q_half = gather_plane(q_pair, "rows_1", "rows_0").reshape(-1, half)
    inv_half = gather_plane(inv_pair, "rows_0", "rows_1").reshape(-1, half)
    q_other, inv_other = shift(q_half, CORE, 1), shift(inv_half, CORE, 1)

    scale = jnp.concatenate([left_factor, 1.0 / left_factor])[:, None]
    own = whitened(core, scale, both, q_half, q_other, inv_half, inv_other)
    white, conj = own[:height], own[height:]

    before = shift(own, COLS, 1)
    behind = shift(own, COLS, -1)
    before_2 = shift(before, COLS, 1)
    behind_2 = shift(behind, COLS, -1)

    def pair(left, right):
        signed = jnp.concatenate([right[:height], -right[height:]], axis=0)
        return with_layout_constraint(dot(left, signed, 0, 0), Layout(major_to_minor=(0, 1)))

    def over_cores(pairs):
        products = []
        for a, b in pairs:
            products.append(pair(a, b))
        part = jnp.concatenate(products, axis=1)
        keep = lax.dynamic_slice_in_dim(part, core * half, half, axis=0)
        give = lax.dynamic_slice_in_dim(part, (1 - core) * half, half, axis=0).astype(bf16)
        got = shift(give, CORE, 1)
        part = (keep + got.astype(f32)).astype(bf16)
        return part.reshape(n_plane, piece, part.shape[1])

    def over_plane(part):
        parts = lax.all_to_all(part, PLANE, 0, 0, tiled=True)
        return jnp.sum(parts.astype(f32), axis=0)

    early_part = over_cores([(own, own), (own, behind)])
    early = over_plane(early_part)
    white_f, conj_f = white.astype(f32), conj.astype(f32)
    left_part = jnp.sum(white_f * white_f - conj_f * conj_f, axis=1)
    left_parts = from_everyone(left_part.reshape(-1, 128), COLS)
    left_grad = jnp.sum(left_parts, axis=0).reshape(height)
    top_l = jnp.max(jnp.abs(left_grad))
    before_2, behind_2, _ = lax.optimization_barrier((before_2, behind_2, early_part))
    late_part = over_cores([(before, behind), (before, behind_2), (before_2, behind_2)])
    late = over_plane(late_part)


    q_all = lax.all_gather(after(q_low, late_part), COLS, axis=0)

    top_r = jnp.maximum(jnp.max(jnp.abs(early)), jnp.max(jnp.abs(late)))
    row, lane = (lax.broadcasted_iota(jnp.int32, (piece, 128), i) for i in range(2))
    terms = split(lax.optimization_barrier(jnp.where(lane < 64, top_r, top_l)))
    note = jnp.where(row == 0, terms[0], jnp.where(row == 1, terms[1], terms[2]))
    pieces = jnp.concatenate([early.astype(bf16), late.astype(bf16), note.astype(bf16)], axis=1)
    mine = from_everyone(pieces, PLANE)
    notes = mine[:, :, 5 * width :].astype(f32)
    tops = jnp.max((notes[:, 0:1] + notes[:, 1:2]) + notes[:, 2:3], axis=0)
    tops = from_everyone(jnp.broadcast_to(tops, (8, 128)), (CORE, COLS))
    mine = mine[:, :, : 5 * width].reshape(half, -1)
    gram = in_core_order(mine, shift(mine, CORE, 1), 0)

    def block(i, size=1):
        return gram[:, i * width : (i + size) * width]

    def times(i, by):
        rows = [lax.dynamic_index_in_dim(q_all, (me + j + n_cols) % n_cols, 0, keepdims=False) for j in by]
        return dot(block(i, len(by)), jnp.concatenate(rows, axis=0), 1, 0)

    def turned_times(i, by):
        rows = lax.dynamic_index_in_dim(q_all, (me + by + n_cols) % n_cols, 0, keepdims=False)
        return dot(block(i), rows, 0, 0)

    def sent(value, by):
        return shift(value.astype(bf16), COLS, by).astype(f32)

    values = [turned_times(3, -1), times(4, (2,)), times(2, (1, 2)), turned_times(1, 0) + turned_times(2, -1)]
    got = [sent(value, by) for value, by in zip(values, (2, -2, -1, 1), strict=True)]
    product = times(0, (0, 1))
    tops = jnp.max(after(tops, values[3], product), axis=(0, 1))
    scale_r, scale_l = (learn_rate / (tops[i] + epsilon) for i in (0, 64))
    product = product + ((got[0] + got[1]) + (got[2] + got[3]))
    left_new = left_factor - scale_l * left_grad * left_factor
    q_new = q_right - scale_r * product
    return (left_new, q_new)


def solution(mesh):
    finer = Mesh(
        mesh.devices.reshape(4, 4, 2, mesh.shape["cols"]), ("rows_0", "rows_1", "rows_2", "cols")
    )
    in_specs = (P(ROWS, "cols"), P(ROWS, "cols"), P(ROWS), P("cols", ROWS), P("cols", ROWS))
    out_specs = (P(ROWS), P("cols", ROWS))

    return jax.shard_map(body, mesh=finer, in_specs=in_specs, out_specs=out_specs, check_vma=False)
```
